128 devices in a mesh: owner: 8 (over y, core), rows: 16 (over z, x).
Axes of the slice: x: 4, y: 4, z: 4, core: 2. Of those that a mesh axis runs over, the one named last changes fastest.
Arguments:
- train_gate: float32 [64, 2048, 1024], P('owner', 'rows'), may hold values from -0.1875 to 0.1875
- other_gate: bfloat16 [64, 2048, 1024], P('owner', 'rows'), may hold values from -0.0625 to 0.0625
- train_up: float32 [64, 2048, 1024], P('owner', 'rows'), may hold values from -0.1875 to 0.1875
- other_up: bfloat16 [64, 2048, 1024], P('owner', 'rows'), may hold values from -0.0625 to 0.0625
- train_down: float32 [64, 1024, 2048], P('owner', None, 'rows'), may hold values from -0.25 to 0.25
- other_down: bfloat16 [64, 1024, 2048], P('owner', None, 'rows'), may hold values from -0.09375 to 0.09375
- router_weight: float32 [2048, 64], P('rows', 'owner'), may hold values from -0.125 to 0.125
- router_gain: float32 [2048], P('rows'), may hold values from 0.25 to 1.75
Outputs:
- ready_gate: bfloat16 [64, 2048, 1024], P('owner', None, 'rows')
- ready_up: bfloat16 [64, 2048, 1024], P('owner', None, 'rows')
- ready_down: bfloat16 [64, 1024, 2048], P('owner', 'rows')
- scale_gate: float32 [64, 1024], P('owner', 'rows')
- scale_up: float32 [64, 1024], P('owner', 'rows')
- scale_down: float32 [64, 1024], P('owner', 'rows')
- serve_router: bfloat16 [2048, 64], replicated
The draws below stay inside these ranges and needn't reach their ends.
All inputs are finite; a program needn't handle non-finite values. Where the reference program divides by a largest or mean magnitude, that divisor is 1e-20 or more.
Results may differ from the reference program's by a relative error of at most 0.001.
Values may be sent and summed in bfloat16 or wider, within the bound.
No kernel may reach another device: no remote copies, remote signals or barrier semaphores. Data moves between devices by JAX's collectives and lax.ppermute only.
A program may use at most 128 MiB of HBM per device.

```python
import jax
import jax.numpy as jnp

EXPERTS = 64
D_MODEL = 2048
D_EXPERT = 1024


def strengthened(values, own_key, source, target, parts, factor):
    def block_of(axis_at):
        return (jnp.arange(values.shape[axis_at]) // (values.shape[axis_at] // parts)).reshape((-1,) + (1,) * (values.ndim - 1 - axis_at))

    near = jax.random.permutation(own_key, parts)[block_of(target)]
    far = (block_of(target) + parts // 2) % parts
    return jnp.where((block_of(source) == near) | (block_of(source) == far), factor * values, values)


def shard_levels(key, shape, pieces, least, high):
    def one(dim, blocks):
        steps = jax.random.uniform(jax.random.fold_in(jax.random.fold_in(key, 6), dim), (blocks,), jnp.float32, least / len(pieces), high / len(pieces))
        return jnp.repeat(jnp.exp(steps), shape[dim] // blocks).reshape((-1,) + (1,) * (len(shape) - dim - 1))

    gain = one(*pieces[0])
    for cut in pieces[1:]:
        gain = gain * one(*cut)
    return gain


def bell_draw(own_key, shape, width, most, shards=(), held_as=jnp.bfloat16):
    values = jax.random.normal(own_key, shape, jnp.float32) * width
    if len(shards) > 0:
        values = shard_levels(own_key, shape, shards, -0.22, 0.18) * values
    return jnp.clip(values, min=-most, max=most).astype(held_as)


def gaussian_with(key, shape, deviation, limit, pieces, heavy, dtype=jnp.bfloat16):
    entries = deviation * jax.random.normal(key, shape, jnp.float32)
    if pieces:
        entries = entries * shard_levels(key, shape, pieces, -0.22, 0.18)
    return jnp.clip(strengthened(entries, jax.random.fold_in(key, 3), *heavy), -limit, limit).astype(dtype)


def setup_inputs(seed: int = 0) -> dict:
    key_list = jax.random.split(jax.random.key(seed), 9)
    train_gate = gaussian_with(key_list[0], (EXPERTS, D_MODEL, D_EXPERT), D_MODEL ** -0.5, 0.1875, ((0, 8), (1, 16)), (1, 2, 16, 2.0), jnp.float32)
    other_gate = bell_draw(key_list[1], (EXPERTS, D_MODEL, D_EXPERT), (D_MODEL * 4) ** -0.5, 0.0625, ((0, 8), (1, 16)))
    train_up = gaussian_with(key_list[2], (EXPERTS, D_MODEL, D_EXPERT), D_MODEL ** -0.5, 0.1875, ((0, 8), (1, 16)), (1, 2, 16, 2.0), jnp.float32)
    other_up = bell_draw(key_list[3], (EXPERTS, D_MODEL, D_EXPERT), (D_MODEL * 4) ** -0.5, 0.0625, ((0, 8), (1, 16)))
    train_down = gaussian_with(key_list[4], (EXPERTS, D_EXPERT, D_MODEL), D_EXPERT ** -0.5, 0.25, ((0, 8), (2, 16)), (2, 1, 16, 2.0), jnp.float32)
    other_down = bell_draw(key_list[5], (EXPERTS, D_EXPERT, D_MODEL), (D_EXPERT * 4) ** -0.5, 0.09375, ((0, 8), (2, 16)))
    router_weight = bell_draw(key_list[6], (D_MODEL, EXPERTS), D_MODEL ** -0.5, 0.125, ((0, 16), (1, 8)), jnp.float32)
    router_gain = jnp.clip(1.0 + 0.15 * jax.random.normal(key_list[7], (D_MODEL,), jnp.float32), 0.25, 1.75)
    return {"train_gate": train_gate, "other_gate": other_gate, "train_up": train_up, "other_up": other_up, "train_down": train_down, "other_down": other_down, "router_weight": router_weight, "router_gain": router_gain}


def reference(train_gate, other_gate, train_up, other_up, train_down, other_down, router_weight, router_gain):
    latest_gate = train_gate + other_gate.astype(jnp.float32)
    latest_up = train_up + other_up.astype(jnp.float32)
    latest_down = train_down + other_down.astype(jnp.float32)
    scale_gate = jnp.max(jnp.abs(latest_gate), axis=1)
    ready_gate = (latest_gate / jnp.expand_dims(scale_gate, 1)).astype(jnp.bfloat16)
    scale_up = jnp.max(jnp.abs(latest_up), axis=1)
    ready_up = (latest_up / jnp.expand_dims(scale_up, 1)).astype(jnp.bfloat16)
    scale_down = jnp.max(jnp.abs(latest_down), axis=2)
    ready_down = (latest_down / jnp.expand_dims(scale_down, 2)).astype(jnp.bfloat16)
    serve_router = (router_weight * router_gain[:, None]).astype(jnp.bfloat16)
    return ready_gate, ready_up, ready_down, scale_gate, scale_up, scale_down, serve_router
```

```python
import functools
import math

import jax
import jax.numpy as jnp
from jax import lax
from jax.experimental import pallas as pl
from jax.experimental.pallas import tpu as pltpu
from jax.sharding import PartitionSpec as P

POWER = 17
GAIN = 2.0 ** (126 / POWER)
ROOT = 1.0 / (POWER * math.log(2.0))
LEAST = 1e-30
TAIL = 48
AHEAD = 3
F32, BF16 = jnp.float32, jnp.bfloat16


def encode(x, inverse):
    y = x * inverse
    power = y * y
    for _ in range(3):
        power = power * power
    return (power * y).astype(BF16)


def decode(code, factor):
    size = (jnp.exp2(jnp.log(jnp.abs(code).astype(F32)) * ROOT) * factor).astype(BF16)
    return jnp.where(code < 0, -size, size)


def in_parts(values):
    high = values.astype(BF16).astype(F32)
    rest = values - high
    middle = rest.astype(BF16).astype(F32)
    return high, middle, rest - middle


def for_peer(values, peer, width):
    at = peer * width // (2 * width) * 2 * width
    tile = values[:, at : at + 2 * width]
    rows = tile.shape[0] // 2
    low, high = tile[:rows], tile[rows:]
    left = lax.broadcasted_iota(jnp.int32, low.shape, 1) < width
    if peer % 2:
        return jnp.where(left, pltpu.roll(low, width, 1), high)
    return jnp.where(left, low, pltpu.roll(high, width, 1))


def send_kernel(peers, gate, d_gate, up, d_up, down, d_down, weight, gain, out, *scratch):
    (gate_in, d_gate_in, up_in, d_up_in, down_in, d_down_in) = scratch[:6]
    staged, most_gate, most_up, most_down, arrived, left = scratch[6:]
    experts, columns, lanes = down.shape
    width = columns // peers
    pairs = experts * width
    total = 3 * pairs

    def incoming(k, expert):
        source = (down, d_down, gate, d_gate, up, d_up)[k]
        target = (down_in, d_down_in, gate_in, d_gate_in, up_in, d_up_in)[k]
        return pltpu.make_async_copy(source.at[expert], target.at[expert], arrived.at[k, expert])

    def outgoing(k, first, rows, at):
        part = (slice(None), pl.ds(first, rows))
        return pltpu.make_async_copy(staged.at[part], out.at[part], left.at[k, at])

    for expert in range(AHEAD):
        for k in range(6):
            incoming(k, expert).start()

    lane = lax.broadcasted_iota(jnp.int32, most_down.shape, 1)

    def one(expert, carry):
        first = pl.multiple_of(expert * width, width)

        @pl.when(expert + AHEAD < experts)
        def _():
            for k in range(6):
                incoming(k, expert + AHEAD).start()

        incoming(0, expert).wait()
        incoming(1, expert).wait()
        x = down_in[expert] + d_down_in[expert].astype(F32)
        most = jnp.maximum(jnp.max(jnp.abs(x), axis=1, keepdims=True), LEAST)
        code = encode(x, GAIN / most)
        staged[:, pl.ds(first, width), :] = code.reshape(peers, width, lanes)
        most_down[...] = jnp.where(lane == expert, most, most_down[...])
        outgoing(0, first, width, expert).start()
        for k, (train, other, held) in enumerate(
            ((gate_in, d_gate_in, most_gate), (up_in, d_up_in, most_up))
        ):
            incoming(2 + 2 * k, expert).wait()
            incoming(3 + 2 * k, expert).wait()
            x = train[expert] + other[expert].astype(F32)
            most = jnp.maximum(jnp.max(jnp.abs(x), axis=0, keepdims=True), LEAST)
            code = encode(x, GAIN / most).T
            at = pl.multiple_of(pairs + expert * 2 * width + k * width, width)
            staged[:, pl.ds(at, width), :] = code.reshape(peers, width, lanes)
            held[pl.ds(expert, 1), :] = most
        outgoing(1, pl.multiple_of(pairs + expert * 2 * width, width), 2 * width, expert).start()
        return carry

    lax.fori_loop(0, experts, one, 0)
    parts = tuple(
        zip(*(in_parts(v) for v in (most_down[...].T[:8], most_gate[...], most_up[...])))
    )
    router = weight[...] * gain[...]
    for peer in range(peers):
        rows = [for_peer(part, peer, width) for split in parts for part in split]
        rows = jnp.concatenate([*rows, jnp.zeros_like(rows[0]), router], axis=0)
        staged[peer, total:, :] = rows.astype(BF16)
    outgoing(0, total, TAIL, experts).start()
    for expert in range(experts):
        outgoing(0, expert * width, width, expert).wait()
        outgoing(1, pairs + expert * 2 * width, 2 * width, expert).wait()
    outgoing(0, total, TAIL, experts).wait()


def factors(parts, table, scale):
    peers, rows, lanes = parts.shape
    half = lanes // 2
    for row in range(rows):
        local = parts[:, row, :]
        most = jnp.max(local, axis=0, keepdims=True)
        scale[row : row + 1, :] = most[:, :half]
        scale[row + rows : row + rows + 1, :] = pltpu.roll(most, half, 1)[:, :half]
        factor = local * ((1.0 / GAIN) / most)
        factor = jnp.concatenate([factor, jnp.zeros((lanes - peers, lanes), F32)], axis=0)
        table[row] = factor.T


def spread(codes, expert, first, width, table, out):
    rows = table.shape[0]
    half = pl.multiple_of(lax.div(expert, rows) * width, width)
    factor = table[lax.rem(expert, rows), pl.ds(half, width), :]
    for peer in range(codes.shape[1]):
        got = codes[expert, peer, first : first + width, :]
        out[expert, :, peer * 128 : (peer + 1) * 128] = decode(got, factor[:, peer : peer + 1])


def take_kernel(first, count, got, *refs):
    outs, scales = refs[:count], refs[count : 2 * count]
    extra = refs[2 * count : -(2 * count + 5)]
    codes, tail = refs[-(2 * count + 5) : -(2 * count + 3)]
    tables, staged = refs[-(2 * count + 3) : -(count + 3)], refs[-(count + 3) : -3]
    arrived, left, tailed = refs[-3:]
    experts, peers, rows, lanes = codes.shape
    width = rows // count

    def incoming(expert):
        start = expert * rows + first
        return pltpu.make_async_copy(
            got.at[:, pl.ds(start, rows)], codes.at[expert], arrived.at[expert]
        )

    def outgoing(k, expert):
        return pltpu.make_async_copy(staged[k].at[expert], outs[k].at[expert], left.at[k, expert])

    last = pltpu.make_async_copy(got.at[:, pl.ds(3 * experts * width, TAIL)], tail, tailed)
    last.start()
    for expert in range(AHEAD):
        incoming(expert).start()
    last.wait()
    ends = tail[...].astype(F32)
    for k in range(count):
        at = 4 * (k + (count > 1))
        local = ends[:, at : at + 4] + ends[:, at + 12 : at + 16] + ends[:, at + 24 : at + 28]
        factors(local, tables[k], scales[k])
    for router in extra:
        for peer in range(peers):
            row = ends[peer, TAIL - 8 :].astype(BF16)
            for owner in range(router.shape[0]):
                router[owner, :, peer * lanes : (peer + 1) * lanes] = row

    def one(expert, carry):
        @pl.when(expert + AHEAD < experts)
        def _():
            incoming(expert + AHEAD).start()

        incoming(expert).wait()
        for k in range(count):
            spread(codes, expert, k * width, width, tables[k], staged[k])
            outgoing(k, expert).start()
        return carry

    lax.fori_loop(0, experts, one, 0)
    for expert in range(experts):
        for k in range(count):
            outgoing(k, expert).wait()


def cost(elements, operations):
    return pl.CostEstimate(flops=elements * operations, bytes_accessed=elements * 8, transcendentals=0)


ANY = pl.BlockSpec(memory_space=pl.ANY)
WHOLE = pl.BlockSpec(memory_space=pltpu.VMEM)
DMA = pltpu.SemaphoreType.DMA


def send(arrays, weight, gain, peers):
    experts, columns, lanes = arrays[4].shape
    rows = 3 * experts * columns // peers + TAIL
    return pl.pallas_call(
        functools.partial(send_kernel, peers),
        in_specs=[ANY] * 6 + [WHOLE] * 2,
        out_specs=ANY,
        out_shape=jax.ShapeDtypeStruct((peers, rows, lanes), BF16),
        scratch_shapes=[
            *(pltpu.VMEM(a.shape, a.dtype) for a in arrays),
            pltpu.VMEM((peers, rows, lanes), BF16),
            pltpu.VMEM((experts, columns), F32),
            pltpu.VMEM((experts, columns), F32),
            pltpu.VMEM((columns, lanes), F32),
            DMA((6, experts)),
            DMA((2, experts + 1)),
        ],
        cost_estimate=cost(3 * arrays[4].size, 20),
        name="send",
    )(*arrays, weight, gain)


def take(got, first, count, owners, experts, width):
    peers, _, lanes = got.shape
    out = jax.ShapeDtypeStruct((experts, width, peers * lanes), BF16)
    scale = jax.ShapeDtypeStruct((experts, width), F32)
    router = [jax.ShapeDtypeStruct((owners, 8, peers * lanes), BF16)] if owners else []
    return pl.pallas_call(
        functools.partial(take_kernel, first, count),
        in_specs=[ANY],
        out_specs=[ANY] * count + [WHOLE] * (count + len(router)),
        out_shape=[out] * count + [scale] * count + router,
        scratch_shapes=[
            pltpu.VMEM((experts, peers, count * width, lanes), BF16),
            pltpu.VMEM((peers, TAIL, lanes), BF16),
            *[pltpu.VMEM((4, lanes, lanes), F32)] * count,
            *[pltpu.VMEM((experts, width, peers * lanes), BF16)] * count,
            DMA((experts,)),
            DMA((count, experts)),
            DMA(()),
        ],
        cost_estimate=cost(count * experts * width * peers * lanes, 20),
        name="take_pair" if count > 1 else "take_down",
    )(got)


def exchange(array, axis):
    return lax.all_to_all(array, axis, 0, 0, tiled=True)


def shards(
    train_gate, other_gate, train_up, other_up, train_down, other_down, router_weight, router_gain
):
    peers, owners = lax.axis_size("rows"), lax.axis_size("owner")
    experts, columns, _ = train_down.shape
    width = columns // peers
    arrays = (train_gate, other_gate, train_up, other_up, train_down, other_down)
    got = exchange(send(arrays, router_weight.T, router_gain[None, :], peers), "rows")
    ready_down, scale_down, router = take(got, 0, 1, owners, experts, width)
    router = exchange(router, "owner")
    gate, up, scale_gate, scale_up = take(got, experts * width, 2, 0, experts, width)
    serve_router = router.reshape(-1, router.shape[2]).T
    ready_gate, ready_up = jnp.swapaxes(gate, 1, 2), jnp.swapaxes(up, 1, 2)
    return (ready_gate, ready_up, ready_down, scale_gate, scale_up, scale_down, serve_router)


def solution(mesh):
    placed = (
        P("owner", "rows", None),
        P("owner", "rows", None),
        P("owner", "rows", None),
        P("owner", "rows", None),
        P("owner", None, "rows"),
        P("owner", None, "rows"),
        P("rows", "owner"),
        P("rows"),
    )
    return jax.shard_map(
        shards,
        mesh=mesh,
        in_specs=placed,
        out_specs=(
            P("owner", None, "rows"),
            P("owner", None, "rows"),
            P("owner", "rows", None),
            P("owner", "rows"),
            P("owner", "rows"),
            P("owner", "rows"),
            P(),
        ),
        check_vma=False,
    )
```

```python
import functools
import math

import jax
import jax.numpy as jnp
from jax import lax
from jax.experimental import pallas as pl
from jax.experimental.pallas import tpu as pltpu
from jax.sharding import PartitionSpec as P

POWER = 17
GAIN = 2.0 ** (126 / POWER)
ROOT = (1.0 / POWER - 1.0) / math.log(2.0)
TINY = 2.0**-126
LEAST = 1e-30
TAIL = 48
AHEAD = 2
F32, BF16 = jnp.float32, jnp.bfloat16


def encode(x, inverse):
    y = x * inverse
    power = y * y
    for _ in range(3):
        power = power * power
    return (power * y).astype(BF16)


def decode(code, factor):
    code = code.astype(F32)
    size = jnp.maximum(jnp.abs(code), TINY)
    return (jnp.exp2(jnp.log(size) * ROOT) * code * factor).astype(BF16)


def in_parts(values):
    high = values.astype(BF16).astype(F32)
    rest = values - high
    middle = rest.astype(BF16).astype(F32)
    return high, middle, rest - middle


def for_peer(values, peer, width):
    at = peer * width // (2 * width) * 2 * width
    tile = values[:, at : at + 2 * width]
    rows = tile.shape[0] // 2
    low, high = tile[:rows], tile[rows:]
    left = lax.broadcasted_iota(jnp.int32, low.shape, 1) < width
    if peer % 2:
        return jnp.where(left, pltpu.roll(low, width, 1), high)
    return jnp.where(left, low, pltpu.roll(high, width, 1))


def send_kernel(peers, gate, d_gate, up, d_up, down, d_down, weight, gain, out, *scratch):
    (gate_in, d_gate_in, up_in, d_up_in, down_in, d_down_in) = scratch[:6]
    most_gate, most_up, most_down, weight_in, gain_in, arrived, small = scratch[6:]
    experts, columns, lanes = down.shape
    width = columns // peers
    pairs = experts * width
    total = 3 * pairs

    def incoming(k, expert):
        source = (down, d_down, gate, d_gate, up, d_up)[k]
        target = (down_in, d_down_in, gate_in, d_gate_in, up_in, d_up_in)[k]
        return pltpu.make_async_copy(source.at[expert], target.at[expert], arrived.at[k, expert])

    for expert in range(AHEAD):
        for k in range(6):
            incoming(k, expert).start()
    load_weight = pltpu.make_async_copy(weight, weight_in, small.at[0])
    load_gain = pltpu.make_async_copy(gain, gain_in, small.at[1])
    load_weight.start()
    load_gain.start()
    lane = lax.broadcasted_iota(jnp.int32, (width, lanes), 1)
    row = lax.broadcasted_iota(jnp.int32, (experts, lanes), 0)

    def one(expert, carry):
        first = pl.multiple_of(expert * width, width)

        @pl.when(expert + AHEAD < experts)
        def _():
            for k in range(6):
                incoming(k, expert + AHEAD).start()

        incoming(0, expert).wait()
        incoming(1, expert).wait()
        for peer in range(peers):
            part = slice(peer * width, (peer + 1) * width)
            x = down_in[expert, part, :] + d_down_in[expert, part, :].astype(F32)
            most = jnp.maximum(jnp.max(jnp.abs(x), axis=1, keepdims=True), LEAST)
            out[peer, pl.ds(first, width), :] = encode(x, GAIN / most)
            most_down[part, :] = jnp.where(lane == expert, most, most_down[part, :])
        for k, (train, other, held) in enumerate(
            ((gate_in, d_gate_in, most_gate), (up_in, d_up_in, most_up))
        ):
            incoming(2 + 2 * k, expert).wait()
            incoming(3 + 2 * k, expert).wait()
            at = pl.multiple_of(pairs + expert * 2 * width + k * width, width)
            for pair in range(peers // 2):
                part = slice(pair * lanes, (pair + 1) * lanes)
                x = train[expert, :, part] + other[expert, :, part].astype(F32)
                most = jnp.maximum(jnp.max(jnp.abs(x), axis=0, keepdims=True), LEAST)
                code = encode(x, GAIN / most).T
                out[2 * pair, pl.ds(at, width), :] = code[:width]
                out[2 * pair + 1, pl.ds(at, width), :] = code[width:]
                held[:, part] = jnp.where(row == expert, most, held[:, part])
        return carry

    lax.fori_loop(0, experts, one, 0)
    parts = tuple(
        zip(*(in_parts(v) for v in (most_down[...].T[:8], most_gate[...], most_up[...])))
    )
    load_weight.wait()
    load_gain.wait()
    router = weight_in[...] * gain_in[...]
    for peer in range(peers):
        rows = [for_peer(part, peer, width) for split in parts for part in split]
        rows = jnp.concatenate([*rows, jnp.zeros_like(rows[0]), router], axis=0)
        out[peer, total:, :] = rows.astype(BF16)


def factors(parts, table, scale):
    peers, rows, lanes = parts.shape
    half = lanes // 2
    for row in range(rows):
        local = parts[:, row, :]
        most = jnp.max(local, axis=0, keepdims=True)
        scale[row : row + 1, :] = most[:, :half]
        scale[row + rows : row + rows + 1, :] = pltpu.roll(most, half, 1)[:, :half]
        factor = local * ((1.0 / GAIN) / most)
        factor = jnp.concatenate([factor, jnp.zeros((lanes - peers, lanes), F32)], axis=0)
        table[row] = factor.T


def copies_kernel(tile, router):
    lanes = tile.shape[2]
    for peer in range(tile.shape[0]):
        for owner in range(router.shape[0]):
            router[owner, :, peer * lanes : (peer + 1) * lanes] = tile[peer]


def take_kernel(got, *refs):
    outs, scales, codes, tail = refs[:3], refs[3:6], refs[6], refs[7]
    tables, staged, scaled = refs[8:11], refs[11:14], refs[14:17]
    arrived, left, tailed, scaling = refs[17:]
    experts, peers, rows, lanes = codes.shape
    width = rows // 3

    def incoming(k, expert):
        start = expert * width if k == 0 else (experts + 2 * expert) * width
        size, to = (width, 0) if k == 0 else (2 * width, width)
        return pltpu.make_async_copy(
            got.at[:, pl.ds(pl.multiple_of(start, width), size)],
            codes.at[expert, :, pl.ds(to, size)],
            arrived.at[k, expert],
        )

    def outgoing(k, expert):
        return pltpu.make_async_copy(staged[k].at[expert], outs[k].at[expert], left.at[k, expert])

    last = pltpu.make_async_copy(got.at[:, pl.ds(experts * rows, TAIL)], tail, tailed)
    last.start()
    for expert in range(AHEAD):
        incoming(0, expert).start()
        incoming(1, expert).start()
    last.wait()
    ends = tail[...].astype(F32)
    for k in range(3):
        at = 4 * k
        local = ends[:, at : at + 4] + ends[:, at + 12 : at + 16] + ends[:, at + 24 : at + 28]
        factors(local, tables[k], scaled[k])
    scalings = [pltpu.make_async_copy(scaled[k], scales[k], scaling.at[k]) for k in range(3)]
    for copy in scalings:
        copy.start()

    def one(expert, carry):
        @pl.when(expert + AHEAD < experts)
        def _():
            incoming(0, expert + AHEAD).start()
            incoming(1, expert + AHEAD).start()

        half = pl.multiple_of(lax.div(expert, 4) * width, width)
        for k in range(3):
            if k < 2:
                incoming(k, expert).wait()
            factor = tables[k][lax.rem(expert, 4), pl.ds(half, width), :]
            for peer in range(peers):
                code = codes[expert, peer, k * width : (k + 1) * width, :]
                staged[k][expert, :, peer * lanes : (peer + 1) * lanes] = decode(
                    code, factor[:, peer : peer + 1]
                )
            outgoing(k, expert).start()
        return carry

    lax.fori_loop(0, experts, one, 0)
    for expert in range(experts):
        for k in range(3):
            outgoing(k, expert).wait()
    for copy in scalings:
        copy.wait()


def cost(elements, operations):
    return pl.CostEstimate(flops=elements * operations, bytes_accessed=elements * 8, transcendentals=0)


HBM = pl.BlockSpec(memory_space=pltpu.HBM)
WHOLE = pl.BlockSpec(memory_space=pltpu.VMEM)
DMA = pltpu.SemaphoreType.DMA


def in_hbm(array):
    return pltpu.with_memory_space_constraint(array, pltpu.HBM)


def send(arrays, weight, gain, peers):
    experts, columns, lanes = arrays[4].shape
    rows = 3 * experts * columns // peers + TAIL
    return pl.pallas_call(
        functools.partial(send_kernel, peers),
        in_specs=[HBM] * 8,
        out_specs=WHOLE,
        out_shape=pltpu.VMEM((peers, rows, lanes), BF16),
        scratch_shapes=[
            *(pltpu.VMEM(a.shape, a.dtype) for a in arrays),
            pltpu.VMEM((experts, columns), F32),
            pltpu.VMEM((experts, columns), F32),
            pltpu.VMEM((columns, lanes), F32),
            pltpu.VMEM(weight.shape, F32),
            pltpu.VMEM(gain.shape, F32),
            DMA((6, experts)),
            DMA((2,)),
        ],
        compiler_params=pltpu.CompilerParams(vmem_limit_bytes=32 << 20),
        cost_estimate=cost(3 * arrays[4].size, 20),
        name="send",
    )(*(in_hbm(a) for a in (*arrays, weight, gain)))


def copies(got, owners):
    peers, rows, lanes = got.shape
    return pl.pallas_call(
        copies_kernel,
        grid=(1,),
        in_specs=[pl.BlockSpec((peers, 8, lanes), lambda i: (0, rows // 8 - 1, 0))],
        out_specs=WHOLE,
        out_shape=jax.ShapeDtypeStruct((owners, 8, peers * lanes), BF16),
        name="copies",
    )(in_hbm(got))


def take(got, experts, width):
    peers, _, lanes = got.shape
    shape = (experts, width, peers * lanes)
    return pl.pallas_call(
        take_kernel,
        in_specs=[HBM],
        out_specs=[HBM] * 6,
        out_shape=[jax.ShapeDtypeStruct(shape, BF16)] * 3
        + [jax.ShapeDtypeStruct((experts, width), F32)] * 3,
        scratch_shapes=[
            pltpu.VMEM((experts, peers, 3 * width, lanes), BF16),
            pltpu.VMEM((peers, TAIL, lanes), BF16),
            *[pltpu.VMEM((4, lanes, lanes), F32)] * 3,
            *[pltpu.VMEM(shape, BF16)] * 3,
            *[pltpu.VMEM((experts, width), F32)] * 3,
            DMA((2, experts)),
            DMA((3, experts)),
            DMA(()),
            DMA((3,)),
        ],
        compiler_params=pltpu.CompilerParams(vmem_limit_bytes=58 << 20),
        cost_estimate=cost(3 * experts * width * peers * lanes, 20),
        name="take",
    )(in_hbm(got))


def exchange(array, axis):
    return lax.all_to_all(array, axis, 0, 0, tiled=True)


def shards(
    train_gate, other_gate, train_up, other_up, train_down, other_down, router_weight, router_gain
):
    peers, owners = lax.axis_size("rows"), lax.axis_size("owner")
    experts, columns, _ = train_down.shape
    width = columns // peers
    arrays = (train_gate, other_gate, train_up, other_up, train_down, other_down)
    got = exchange(send(arrays, router_weight.T, router_gain[None, :], peers), "rows")
    router = exchange(copies(got, owners), "owner")
    ready_down, gate, up, scale_down, scale_gate, scale_up = take(got, experts, width)
    serve_router = router.reshape(-1, router.shape[2]).T
    ready_gate, ready_up = jnp.swapaxes(gate, 1, 2), jnp.swapaxes(up, 1, 2)
    return (ready_gate, ready_up, ready_down, scale_gate, scale_up, scale_down, serve_router)


def solution(mesh):
    placed = (
        P("owner", "rows", None),
        P("owner", "rows", None),
        P("owner", "rows", None),
        P("owner", "rows", None),
        P("owner", None, "rows"),
        P("owner", None, "rows"),
        P("rows", "owner"),
        P("rows"),
    )
    return jax.shard_map(
        shards,
        mesh=mesh,
        in_specs=placed,
        out_specs=(
            P("owner", None, "rows"),
            P("owner", None, "rows"),
            P("owner", "rows", None),
            P("owner", "rows"),
            P("owner", "rows"),
            P("owner", "rows"),
            P(),
        ),
        check_vma=False,
    )
```

```python
import functools
import math

import jax
import jax.numpy as jnp
from jax import lax
from jax.experimental import pallas as pl
from jax.experimental.pallas import tpu as pltpu
from jax.sharding import PartitionSpec as P

POWER = 17
GAIN = 2.0 ** (126 / POWER)
ROOT = (1.0 / POWER - 1.0) / math.log(2.0)
TINY = 2.0**-126
LEAST = 1e-30
TAIL = 32
AHEAD = 2
F32, BF16 = jnp.float32, jnp.bfloat16


def encode(x, inverse):
    y = x * inverse
    power = y * y
    for _ in range(3):
        power = power * power
    return (power * y).astype(BF16)


def decode(code, factor):
    code = code.astype(F32)
    size = jnp.maximum(jnp.abs(code), TINY)
    return (jnp.exp2(jnp.log(size) * ROOT) * code * factor).astype(BF16)


def in_parts(values):
    high = values.astype(BF16).astype(F32)
    rest = values - high
    return high, rest.astype(BF16).astype(F32)


def for_peer(values, peer, width):
    at = peer * width // (2 * width) * 2 * width
    tile = values[:, at : at + 2 * width]
    rows = tile.shape[0] // 2
    low, high = tile[:rows], tile[rows:]
    left = lax.broadcasted_iota(jnp.int32, low.shape, 1) < width
    if peer % 2:
        return jnp.where(left, pltpu.roll(low, width, 1), high)
    return jnp.where(left, low, pltpu.roll(high, width, 1))


def send_kernel(peers, gate, d_gate, up, d_up, down, d_down, weight, gain, out, *scratch):
    (gate_in, d_gate_in, up_in, d_up_in, down_in, d_down_in) = scratch[:6]
    most_gate, most_up, most_down, weight_in, gain_in, arrived, small = scratch[6:]
    experts, columns, lanes = down.shape
    width = columns // peers
    pairs = experts * width
    total = 3 * pairs

    def incoming(k, expert):
        source = (down, d_down, gate, d_gate, up, d_up)[k]
        target = (down_in, d_down_in, gate_in, d_gate_in, up_in, d_up_in)[k]
        return pltpu.make_async_copy(source.at[expert], target.at[expert], arrived.at[k, expert])

    for expert in range(AHEAD):
        for k in range(6):
            incoming(k, expert).start()
    load_weight = pltpu.make_async_copy(weight, weight_in, small.at[0])
    load_gain = pltpu.make_async_copy(gain, gain_in, small.at[1])
    load_weight.start()
    load_gain.start()
    lane = lax.broadcasted_iota(jnp.int32, (width, lanes), 1)
    row = lax.broadcasted_iota(jnp.int32, (experts, lanes), 0)

    def one(expert, carry):
        first = pl.multiple_of(expert * width, width)

        @pl.when(expert + AHEAD < experts)
        def _():
            for k in range(6):
                incoming(k, expert + AHEAD).start()

        incoming(0, expert).wait()
        incoming(1, expert).wait()
        for peer in range(peers):
            part = slice(peer * width, (peer + 1) * width)
            x = down_in[expert, part, :] + d_down_in[expert, part, :].astype(F32)
            most = jnp.maximum(jnp.max(jnp.abs(x), axis=1, keepdims=True), LEAST)
            out[peer, pl.ds(first, width), :] = encode(x, GAIN / most)
            most_down[part, :] = jnp.where(lane == expert, most, most_down[part, :])
        for k, (train, other, held) in enumerate(
            ((gate_in, d_gate_in, most_gate), (up_in, d_up_in, most_up))
        ):
            incoming(2 + 2 * k, expert).wait()
            incoming(3 + 2 * k, expert).wait()
            at = pl.multiple_of(pairs + expert * 2 * width + k * width, width)
            for pair in range(peers // 2):
                part = slice(pair * lanes, (pair + 1) * lanes)
                x = train[expert, :, part] + other[expert, :, part].astype(F32)
                most = jnp.maximum(jnp.max(jnp.abs(x), axis=0, keepdims=True), LEAST)
                code = encode(x, GAIN / most).T
                out[2 * pair, pl.ds(at, width), :] = code[:width]
                out[2 * pair + 1, pl.ds(at, width), :] = code[width:]
                held[:, part] = jnp.where(row == expert, most, held[:, part])
        return carry

    lax.fori_loop(0, experts, one, 0)
    parts = tuple(
        zip(*(in_parts(v) for v in (most_down[...].T[:8], most_gate[...], most_up[...])))
    )
    load_weight.wait()
    load_gain.wait()
    router = weight_in[...] * gain_in[...]
    for peer in range(peers):
        rows = [for_peer(part, peer, width) for split in parts for part in split]
        rows = jnp.concatenate([*rows, router], axis=0)
        out[peer, total:, :] = rows.astype(BF16)


def factors(parts, table, scale):
    peers, rows, lanes = parts.shape
    half = lanes // 2
    for row in range(rows):
        local = parts[:, row, :]
        most = jnp.max(local, axis=0, keepdims=True)
        scale[row : row + 1, :] = most[:, :half]
        scale[row + rows : row + rows + 1, :] = pltpu.roll(most, half, 1)[:, :half]
        factor = local * ((1.0 / GAIN) / most)
        factor = jnp.concatenate([factor, jnp.zeros((lanes - peers, lanes), F32)], axis=0)
        table[row] = factor.T


def copies_kernel(tile, router):
    lanes = tile.shape[2]
    for peer in range(tile.shape[0]):
        for owner in range(router.shape[0]):
            router[owner, :, peer * lanes : (peer + 1) * lanes] = tile[peer]


def take_kernel(got, *refs):
    outs, scales, codes, tail = refs[:3], refs[3:6], refs[6], refs[7]
    tables, staged, scaled = refs[8:11], refs[11:14], refs[14:17]
    arrived, left, tailed, scaling = refs[17:]
    experts, peers, rows, lanes = codes.shape
    width = rows // 3

    def incoming(k, expert):
        start = expert * width if k == 0 else (experts + 2 * expert) * width
        size, to = (width, 0) if k == 0 else (2 * width, width)
        return pltpu.make_async_copy(
            got.at[:, pl.ds(pl.multiple_of(start, width), size)],
            codes.at[expert, :, pl.ds(to, size)],
            arrived.at[k, expert],
        )

    def outgoing(k, expert):
        return pltpu.make_async_copy(staged[k].at[expert], outs[k].at[expert], left.at[k, expert])

    last = pltpu.make_async_copy(got.at[:, pl.ds(experts * rows, TAIL)], tail, tailed)
    last.start()
    for expert in range(AHEAD):
        incoming(0, expert).start()
        incoming(1, expert).start()
    last.wait()
    ends = tail[...].astype(F32)
    for k in range(3):
        at = 4 * k
        local = ends[:, at : at + 4] + ends[:, at + 12 : at + 16]
        factors(local, tables[k], scaled[k])
    scalings = [pltpu.make_async_copy(scaled[k], scales[k], scaling.at[k]) for k in range(3)]
    for copy in scalings:
        copy.start()

    def one(expert, carry):
        @pl.when(expert + AHEAD < experts)
        def _():
            incoming(0, expert + AHEAD).start()
            incoming(1, expert + AHEAD).start()

        half = pl.multiple_of(lax.div(expert, 4) * width, width)
        for k in range(3):
            if k < 2:
                incoming(k, expert).wait()
            factor = tables[k][lax.rem(expert, 4), pl.ds(half, width), :]
            for peer in range(peers):
                code = codes[expert, peer, k * width : (k + 1) * width, :]
                staged[k][expert, :, peer * lanes : (peer + 1) * lanes] = decode(
                    code, factor[:, peer : peer + 1]
                )
            outgoing(k, expert).start()
        return carry

    lax.fori_loop(0, experts, one, 0)
    for expert in range(experts):
        for k in range(3):
            outgoing(k, expert).wait()
    for copy in scalings:
        copy.wait()


def cost(elements, operations):
    return pl.CostEstimate(flops=elements * operations, bytes_accessed=elements * 8, transcendentals=0)


HBM = pl.BlockSpec(memory_space=pltpu.HBM)
WHOLE = pl.BlockSpec(memory_space=pltpu.VMEM)
DMA = pltpu.SemaphoreType.DMA


def in_hbm(array):
    return pltpu.with_memory_space_constraint(array, pltpu.HBM)


def send(arrays, weight, gain, peers):
    experts, columns, lanes = arrays[4].shape
    rows = 3 * experts * columns // peers + TAIL
    return pl.pallas_call(
        functools.partial(send_kernel, peers),
        in_specs=[HBM] * 8,
        out_specs=WHOLE,
        out_shape=pltpu.VMEM((peers, rows, lanes), BF16),
        scratch_shapes=[
            *(pltpu.VMEM(a.shape, a.dtype) for a in arrays),
            pltpu.VMEM((experts, columns), F32),
            pltpu.VMEM((experts, columns), F32),
            pltpu.VMEM((columns, lanes), F32),
            pltpu.VMEM(weight.shape, F32),
            pltpu.VMEM(gain.shape, F32),
            DMA((6, experts)),
            DMA((2,)),
        ],
        compiler_params=pltpu.CompilerParams(vmem_limit_bytes=32 << 20),
        cost_estimate=cost(3 * arrays[4].size, 20),
        name="send",
    )(*(in_hbm(a) for a in (*arrays, weight, gain)))


def copies(got, owners):
    peers, rows, lanes = got.shape
    return pl.pallas_call(
        copies_kernel,
        grid=(1,),
        in_specs=[pl.BlockSpec((peers, 8, lanes), lambda i: (0, rows // 8 - 1, 0))],
        out_specs=WHOLE,
        out_shape=jax.ShapeDtypeStruct((owners, 8, peers * lanes), BF16),
        name="copies",
    )(in_hbm(got))


def take(got, experts, width):
    peers, _, lanes = got.shape
    shape = (experts, width, peers * lanes)
    return pl.pallas_call(
        take_kernel,
        in_specs=[HBM],
        out_specs=[HBM] * 6,
        out_shape=[jax.ShapeDtypeStruct(shape, BF16)] * 3
        + [jax.ShapeDtypeStruct((experts, width), F32)] * 3,
        scratch_shapes=[
            pltpu.VMEM((experts, peers, 3 * width, lanes), BF16),
            pltpu.VMEM((peers, TAIL, lanes), BF16),
            *[pltpu.VMEM((4, lanes, lanes), F32)] * 3,
            *[pltpu.VMEM(shape, BF16)] * 3,
            *[pltpu.VMEM((experts, width), F32)] * 3,
            DMA((2, experts)),
            DMA((3, experts)),
            DMA(()),
            DMA((3,)),
        ],
        compiler_params=pltpu.CompilerParams(vmem_limit_bytes=58 << 20),
        cost_estimate=cost(3 * experts * width * peers * lanes, 20),
        name="take",
    )(in_hbm(got))


def exchange(array, axis):
    return lax.all_to_all(array, axis, 0, 0, tiled=True)


def shards(
    train_gate, other_gate, train_up, other_up, train_down, other_down, router_weight, router_gain
):
    peers, owners = lax.axis_size("rows"), lax.axis_size("owner")
    experts, columns, _ = train_down.shape
    width = columns // peers
    arrays = (train_gate, other_gate, train_up, other_up, train_down, other_down)
    got = exchange(send(arrays, router_weight.T, router_gain[None, :], peers), "rows")
    router = exchange(copies(got, owners), "owner")
    ready_down, gate, up, scale_down, scale_gate, scale_up = take(got, experts, width)
    serve_router = router.reshape(-1, router.shape[2]).T
    ready_gate, ready_up = jnp.swapaxes(gate, 1, 2), jnp.swapaxes(up, 1, 2)
    return (ready_gate, ready_up, ready_down, scale_gate, scale_up, scale_down, serve_router)


def solution(mesh):
    placed = (
        P("owner", "rows", None),
        P("owner", "rows", None),
        P("owner", "rows", None),
        P("owner", "rows", None),
        P("owner", None, "rows"),
        P("owner", None, "rows"),
        P("rows", "owner"),
        P("rows"),
    )
    return jax.shard_map(
        shards,
        mesh=mesh,
        in_specs=placed,
        out_specs=(
            P("owner", None, "rows"),
            P("owner", None, "rows"),
            P("owner", "rows", None),
            P("owner", "rows"),
            P("owner", "rows"),
            P("owner", "rows"),
            P(),
        ),
        check_vma=False,
    )
```
